32 devices in a mesh: lat: 4 (over y, x), lon: 8 (over z, core).
Axes of the slice: x: 2, y: 2, z: 4, core: 2. Of those that a mesh axis runs over, the one named last changes fastest.
Arguments:
- tracers: float32 [64, 1440, 1536], P('lat', 'lon'), may hold values from 0.05 to 9, as said below
- winds: float32 [64, 1440, 32], P('lat', 'lon'), may hold values from -0.16 to 0.16
- row_mask: int32 [64], P('lat'), may hold values from 0 to 1, as said below
- coag_rate: float32 [16], replicated, may hold values from 0.05 to 0.3
- growth_rate: float32 [16], replicated, may hold values from 0.05 to 0.3
Outputs:
- updated: float32 [64, 1440, 1536], P('lat', 'lon')
The draws below stay inside these ranges and needn't reach their ends.
Inputs may be any that keep to these rules, and one draw needn't show every extreme that they name: `tracers`: per cell, mode and level the six channels are M_k = N exp(k mu + k^2 s^2 / 2), k = 0..5, with N in 0.3 to 3, mu in -0.5 to -0.2 and s in 0.25 to 0.4. `row_mask`: 1 on the first K rows (those nearest the pole) and 0 elsewhere, with 8 <= K <= 24.
All inputs are finite; a program needn't handle non-finite values.
Results may differ from the reference program's by a relative error of at most 0.00005.
Values sent between devices are 32-bit elements; how exact they have to be, the bound alone decides.
No kernel may reach another device: no remote copies, remote signals or barrier semaphores. Data moves between devices by JAX's collectives and lax.ppermute only.
A program may use at most 192 MiB of HBM per device.

```python
import math
import jax
import jax.numpy as jnp
from jax import lax

NLON = 1440
GLOBE_ROWS = 720
LEV = 16
MODES = 16
MOMENTS = 6
NLAT = 64


def draw_tracers(key, part):
    key_count, key_centre, key_spread = jax.random.split(jax.random.fold_in(key, 11), 3)
    cells = (NLAT, NLON, MODES * LEV)
    amount = jnp.exp(jax.random.uniform(key_count, cells, jnp.float32, math.log(0.5), math.log(2.0)))
    centre = jax.random.uniform(key_centre, cells, jnp.float32, -0.45, -0.25)
    spread = jax.random.uniform(key_spread, cells, jnp.float32, 0.25, 0.38)
    pieces = [amount * jnp.exp(degree * centre + 0.5 * degree * degree * spread * spread) for degree in range(MOMENTS)]
    return jnp.concatenate(pieces, axis=2).astype(jnp.float32)


def draw_row_mask(key, part):
    cutoff = jax.random.randint(jax.random.fold_in(key, 5), (), NLAT // 8, 3 * NLAT // 8 + 1)
    places = jnp.arange(NLAT, dtype=jnp.int32)
    return (places < cutoff).astype(jnp.int32)


def block_scale(key, extent, shards, least, largest):
    gain, own = 1.0, jax.random.fold_in(key, 6)
    for position, blocks in shards:
        draws = jnp.exp(jax.random.uniform(jax.random.fold_in(own, position), (blocks,), jnp.float32, least / len(shards), largest / len(shards)))
        gain = gain * jnp.repeat(draws, extent[position] // blocks).reshape([-1 if axis == position else 1 for axis in range(len(extent))])
    return gain


def setup_inputs(seed: int = 0) -> dict:
    key_list = jax.random.split(jax.random.key(seed), 6)
    return {
        "tracers": draw_tracers(jax.random.fold_in(key_list[5], 71), 0),
        "winds": jnp.clip(jax.random.uniform(key_list[1], (NLAT, NLON, 2 * LEV), jnp.float32, -0.16, 0.16) * block_scale(key_list[1], (NLAT, NLON, 2 * LEV), ((0, 4), (1, 8)), -0.4, 0.0), -0.16, 0.16),
        "row_mask": draw_row_mask(jax.random.fold_in(key_list[5], 71), 0),
        "coag_rate": jnp.clip(jnp.exp(jax.random.uniform(key_list[3], (MODES,), jnp.float32, math.log(0.05), math.log(0.3))), 0.05, 0.3),
        "growth_rate": jnp.clip(jnp.exp(jax.random.uniform(key_list[4], (MODES,), jnp.float32, math.log(0.05), math.log(0.3))), 0.05, 0.3),
    }


CUT_COSINE = math.cos(math.pi / 4.0)

def row_angles(places):
    return (-90.0 + 180.0 * (places.astype(jnp.float32) + 0.5) / GLOBE_ROWS) * (math.pi / 180.0)

def damping(angles, length):
    waves = jnp.arange(length // 2 + 1, dtype=jnp.float32)
    sines = jnp.sin(waves * (math.pi / length))
    cosines = jnp.cos(angles)[:, None]
    return cosines / jnp.maximum(CUT_COSINE * sines[None, :], cosines)

def moment_sources(moments, coag, growth):
    zeroth, first, second, third, fourth, fifth = moments
    alpha_zero = first / zeroth
    sigma_one = second - alpha_zero * first
    sigma_two = third - alpha_zero * second
    sigma_three = fourth - alpha_zero * third
    sigma_four = fifth - alpha_zero * fourth
    alpha_one = sigma_two / sigma_one - first / zeroth
    beta_one = sigma_one / zeroth
    upper_two = sigma_three - alpha_one * sigma_two - beta_one * second
    upper_three = sigma_four - alpha_one * sigma_three - beta_one * third
    alpha_two = upper_three / upper_two - sigma_two / sigma_one
    beta_two = upper_two / sigma_one
    link_one = jnp.sqrt(beta_one)
    link_two = jnp.sqrt(beta_two)
    centre = (alpha_zero + alpha_one + alpha_two) / 3.0
    shift_zero = alpha_zero - centre
    shift_one = alpha_one - centre
    shift_two = alpha_two - centre
    radius = jnp.sqrt((shift_zero * shift_zero + shift_one * shift_one + shift_two * shift_two + 2.0 * (beta_one + beta_two)) / 6.0)
    scaled_zero = shift_zero / radius
    scaled_one = shift_one / radius
    scaled_two = shift_two / radius
    ratio_one = beta_one / (radius * radius)
    ratio_two = beta_two / (radius * radius)
    half_det = 0.5 * (scaled_zero * (scaled_one * scaled_two - ratio_two) - ratio_one * scaled_two)
    angle = jnp.arccos(jnp.clip(half_det, -1.0, 1.0)) / 3.0
    top_node = centre + 2.0 * radius * jnp.cos(angle)
    low_node = centre + 2.0 * radius * jnp.cos(angle + 2.0 * math.pi / 3.0)
    mid_node = 3.0 * centre - top_node - low_node
    abscissae = (top_node, mid_node, low_node)
    weights = []
    for node in abscissae:
        poly_one = (node - alpha_zero) / link_one
        poly_two = ((node - alpha_one) * poly_one - link_one) / link_two
        weights.append(zeroth / (1.0 + poly_one * poly_one + poly_two * poly_two))
    volumes = [node * node * node for node in abscissae]
    results = []
    for degree in range(6):
        merged = jnp.zeros_like(zeroth)
        for source in range(3):
            for target in range(3):
                joined = volumes[source] + volumes[target]
                change = jnp.exp(degree / 3.0 * jnp.log(joined)) - abscissae[source] ** degree - abscissae[target] ** degree
                merged = merged + weights[source] * weights[target] * joined * change
        growth_sum = jnp.zeros_like(zeroth)
        if degree > 0:
            for source in range(3):
                growth_sum = growth_sum + weights[source] * abscissae[source] ** (degree - 1) / (1.0 + abscissae[source])
            growth_sum = degree * growth * growth_sum
        results.append(moments[degree] + 0.5 * coag * merged + growth_sum)
    return tuple(results)

def polar_filter(winds, row_mask):
    factor = damping(row_angles(jnp.arange(NLAT, dtype=jnp.int32)), NLON)
    spectrum = jnp.fft.rfft(winds, axis=1)
    smooth = jnp.fft.irfft(spectrum * factor[:, :, None], n=NLON, axis=1).astype(jnp.float32)
    return jnp.where(row_mask[:, None, None] > 0, smooth, winds)

def advect(fields, zonal, merid):
    east_value = jnp.roll(fields, -1, axis=1)
    east_wind = jnp.roll(zonal, -1, axis=1)
    zonal_speed = 0.5 * (zonal + east_wind)
    flux_east = jnp.maximum(zonal_speed, 0.0) * fields + jnp.minimum(zonal_speed, 0.0) * east_value
    flux_west = jnp.roll(flux_east, 1, axis=1)
    zero_row = jnp.zeros_like(fields[:1])
    north_value = jnp.concatenate([fields[1:], zero_row], axis=0)
    north_wind = jnp.concatenate([merid[1:], zero_row], axis=0)
    places = jnp.arange(NLAT, dtype=jnp.int32)
    open_face = (places < NLAT - 1).astype(jnp.float32)[:, None, None]
    merid_speed = 0.5 * (merid + north_wind)
    flux_north = (jnp.maximum(merid_speed, 0.0) * fields + jnp.minimum(merid_speed, 0.0) * north_value) * open_face
    flux_south = jnp.concatenate([zero_row, flux_north[:-1]], axis=0)
    return fields - (flux_east - flux_west) - (flux_north - flux_south)

def reference(tracers, winds, row_mask, coag_rate, growth_rate):
    filtered = polar_filter(winds, row_mask)
    zonal = jnp.tile(filtered[:, :, :LEV], (1, 1, MODES))
    merid = jnp.tile(filtered[:, :, LEV:], (1, 1, MODES))
    block_width = MODES * LEV
    advected = [advect(tracers[:, :, degree * block_width:(degree + 1) * block_width], zonal, merid) for degree in range(MOMENTS)]
    coag = jnp.repeat(coag_rate, LEV)
    growth = jnp.repeat(growth_rate, LEV)

    def per_row(row_moments):
        return moment_sources(row_moments, coag, growth)
    updated = lax.map(per_row, tuple(advected))
    return jnp.concatenate(updated, axis=2)
```

```python
import functools
import math

import jax
import jax.numpy as jnp
import numpy as np
from jax import lax
from jax.experimental import pallas as pl
from jax.experimental.pallas import tpu as pltpu
from jax.sharding import PartitionSpec as P


GLOBE_ROWS = 720
LEV = 16
MOMENTS = 6
CUT_COSINE = math.cos(math.pi / 4.0)

LANES = 128
RADIX = 8
GROUP = 12
STEP = 1
EDGE = 8


THIRD_ANGLE = (
    0.8660254823953591,
    0.1666585677307933,
    -0.04797367003362251,
    0.023769973926887133,
    -0.01251053520856182,
    0.005054229492709511,
    -0.0010241076314225976,
)


def round_up(value, step):
    return (value + step - 1) // step * step


def add3(terms):
    return terms[0] + terms[1] + terms[2]


def moment_update(m, coag, growths):
    m0, m1, m2, m3, m4, m5 = m
    r0 = 1.0 / m0
    a0 = m1 * r0
    s1 = m2 - a0 * m1
    s2 = m3 - a0 * m2
    s3 = m4 - a0 * m3
    s4 = m5 - a0 * m4
    r1 = 1.0 / s1
    u = s2 * r1
    a1 = u - a0
    b1 = s1 * r0
    t2 = s3 - a1 * s2 - b1 * m2
    t3 = s4 - a1 * s3 - b1 * m3
    trace = t3 / t2
    a2 = trace - u
    b2 = t2 * r1
    c = trace * (1.0 / 3.0)
    g0 = a0 - c
    g1 = a1 - c
    g2 = a2 - c
    g12 = g1 * g2
    p2 = g0 * g0 - g12 + (b1 + b2)
    rp = lax.rsqrt(p2)
    det = g0 * (g12 - b2) - b1 * g2
    half = det * (rp * rp * rp)
    p = p2 * rp
    full = 1.5 * math.sqrt(3.0)
    size = jnp.minimum(jnp.abs(half), 1.0 / full)
    terms = [k * full**i / math.sqrt(3.0) for i, k in enumerate(THIRD_ANGLE)]
    cosine = terms[-1] * size + terms[-2]
    for k in terms[-3::-1]:
        cosine = cosine * size + k
    square = jnp.maximum(1.0 - 3.0 * (cosine * cosine), 1e-13)
    sine = square * lax.rsqrt(square)
    p = jnp.where(half < 0.0, -p, p)
    g = p * cosine
    e = p * sine
    xa = c + (g + g)
    mid = c - g
    xb = mid + e
    xc = mid - e
    g3 = g + (g + g)
    al = g3 + e
    be = g3 - e
    e2 = e + e
    scale = m0 / (e2 * (al * be))
    da = xa - a0
    db = xb - a0
    dc = xc - a0
    wa = (b1 + db * dc) * (scale * e2)
    wb = (b1 + da * dc) * (scale * al)
    wc = (b1 + da * db) * (scale * be)
    x = (xa, xb, xc)
    w = (wa, wb, wc)

    def mixed3(terms):
        return (terms[0] + terms[2]) - terms[1]

    x2 = [n * n for n in x]
    vol = [n * n2 for n, n2 in zip(x, x2)]
    y2 = [a * b for a, b in zip(w, x2)]
    y4 = [a * b for a, b in zip(y2, x2)]
    y7 = [a * b for a, b in zip(y4, vol)]
    m6 = mixed3([a * b for a, b in zip(y4, x2)])
    m7 = mixed3(y7)
    m8 = mixed3([a * b for a, b in zip(y7, x)])
    z4 = [a * a for a in y2]
    z5 = [a * b for a, b in zip(z4, x)]
    gain1 = add3(z4) * 2.0 ** (1.0 / 3.0)
    gain2 = add3(z5) * 2.0 ** (2.0 / 3.0)
    gain4 = add3([a * b for a, b in zip(z4, vol)]) * 2.0 ** (4.0 / 3.0)
    gain5 = add3([a * b for a, b in zip(z5, vol)]) * 2.0 ** (5.0 / 3.0)
    for i, j in ((0, 2), (0, 1), (1, 2)):
        s = vol[i] + vol[j]
        root = jnp.exp2(jnp.log(s) * (1.0 / (3.0 * math.log(2.0))))
        k1 = (w[i] * w[j]) * s * root
        k2 = k1 * root
        if (i, j) == (0, 2):
            gain1, gain2 = gain1 + k1, gain2 + k2
            gain4, gain5 = gain4 + k1 * s, gain5 + k2 * s
        else:
            gain1, gain2 = gain1 - k1, gain2 - k2
            gain4, gain5 = gain4 - k1 * s, gain5 - k2 * s
    one0 = 1.0 + a0
    one1 = 1.0 + a1
    one2 = 1.0 + a2
    num = one1 * one2 - b2
    grow1 = m0 * num / (one0 * num - b1 * one2)
    grow2 = m0 - grow1
    grow3 = m1 - grow2
    grow4 = m2 - grow3
    grow5 = m3 - grow4
    c0 = coag * m0
    c3 = coag * m3
    keep = 1.0 - c3
    gain3 = c0 * m6 + c3 * m3
    return (
        m0 - c0 * m3,
        (keep * m1 - c0 * m4) + coag * gain1 + growths[0] * grow1,
        (keep * m2 - c0 * m5) + coag * gain2 + growths[1] * grow2,
        m3 + (gain3 - (c0 * m6 + c3 * m3)) + growths[2] * grow3,
        (keep * m4 - c0 * m7) + coag * gain4 + growths[3] * grow4,
        (keep * m5 - c0 * m8) + coag * gain5 + growths[4] * grow5,
    )


class Plan:
    def __init__(self, rows, cols, devices, channels):
        self.rows, self.cols, self.devices, self.channels = rows, cols, devices, channels
        self.series = rows * channels // devices
        self.wide = self.series >= channels
        assert LANES % self.series == 0
        assert devices == 8 if self.wide else (self.series == LEV and devices == 2 * rows)
        self.groups = LANES // self.series
        self.out_rows = pl.cdiv(cols, self.groups)
        self.in_rows = round_up(pl.cdiv(cols + 2, self.groups), 8)
        self.total = cols * devices

    def place(self, row, part):
        if self.wide:
            return row % self.devices, row // self.devices * self.channels + part * LEV
        return row + part * self.rows, 0

    def row_of(self, device, series):
        if self.wide:
            return device + self.devices * (series // self.channels)
        return lax.rem(device, self.rows) + 0 * series


def pack_kernel(plan, place_ref, winds_ref, *refs):
    send_refs, (turned,) = refs[: plan.devices], refs[plan.devices :]
    me = place_ref[0]
    for shift in range(plan.devices):
        dest = lax.rem(me + shift, plan.devices)
        ref = send_refs[shift]
        if plan.wide:
            value = jnp.concatenate(
                [
                    winds_ref[dest + plan.devices * k]
                    for k in range(plan.series // plan.channels)
                ],
                axis=0,
            )
        else:
            whole = winds_ref[lax.rem(dest, plan.rows)]
            value = jnp.where(dest < plan.rows, whole[:LEV], whole[LEV:])
        turned[:, : plan.series] = value.T
        for group in range(plan.groups):
            first = group * plan.out_rows
            count = min(plan.out_rows, plan.cols - first)
            lanes = slice(group * plan.series, (group + 1) * plan.series)
            if count < plan.out_rows:
                ref[:, lanes] = jnp.zeros((plan.out_rows, plan.series), jnp.float32)
            if count > 0:
                ref[:count, lanes] = turned[pl.ds(first, count), : plan.series]


def class_tables(length):
    part = length // RADIX
    pad = round_up(part, 64)
    j = np.arange(part)
    real, mixed = [], []
    waves, repeats = [], []
    for k in (0, RADIX // 2):
        table = np.zeros((pad, pad))
        wave = np.zeros(pad)
        repeat = np.zeros(pad)
        at = 0
        for m in range(k, length // 2 + 1, RADIX):
            angle = 2.0 * np.pi * ((m * j) % length) / length
            single = m in (0, length // 2)
            table[at, :part] = np.cos(angle)
            wave[at], repeat[at] = m, (1.0 if single else 2.0) / length
            at += 1
            if not single:
                table[at, :part] = np.sin(angle)
                wave[at], repeat[at] = m, 2.0 / length
                at += 1
        real.append(table)
        waves.append(wave)
        repeats.append(repeat)
    for k in range(1, RADIX // 2):
        m = RADIX * np.arange(part) + k
        angle = 2.0 * np.pi * ((m[:, None] * j[None, :]) % length) / length
        table = np.zeros((2 * pad, 2 * pad))
        table[:part, :part] = np.cos(angle)
        table[:part, pad : pad + part] = np.sin(angle)
        table[pad : pad + part, :part] = -np.sin(angle)
        table[pad : pad + part, pad : pad + part] = np.cos(angle)
        mixed.append(table)
        wave = np.zeros(pad)
        wave[:part] = np.minimum(m, length - m)
        repeat = np.zeros(pad)
        repeat[:part] = 2.0 / length
        waves.append(wave)
        repeats.append(repeat)
    sines = np.sin(np.stack(waves) * (np.pi / length))

    def halves(tables):
        full = np.stack(tables).astype(np.float32)
        high = full.astype(jnp.bfloat16)
        low = (full - high.astype(np.float32)).astype(jnp.bfloat16)
        return np.stack([high, low], axis=1)

    columns = np.concatenate([sines, np.stack(repeats)], axis=0).T.astype(np.float32)
    return halves(real), halves(mixed), np.ascontiguousarray(columns), pad


def product(table_ref, k, value, transposed):
    high = value.astype(jnp.bfloat16)
    low = (value - high.astype(jnp.float32)).astype(jnp.bfloat16)
    dims = (((0,), (0,)), ((), ())) if transposed else (((1,), (0,)), ((), ()))
    dot = functools.partial(
        lax.dot_general, dimension_numbers=dims, preferred_element_type=jnp.float32
    )
    big = table_ref[k, 0]
    return dot(big, high) + (dot(big, low) + dot(table_ref[k, 1], high))


def filter_kernel(
    plan, pad, place_ref, real_ref, mixed_ref, column_ref, cosine_ref, mask_ref, *refs
):
    devices = plan.devices
    recv_refs, send_refs = refs[:devices], refs[devices : 2 * devices]
    circle, smooth = refs[2 * devices :]
    me = place_ref[0]
    part = plan.total // RADIX
    for shift in range(devices):
        source = lax.rem(me - shift + devices, devices)
        for group in range(plan.groups):
            first = group * plan.out_rows
            count = min(plan.out_rows, plan.cols - first)
            if count <= 0:
                continue
            value = recv_refs[shift][:count, :]
            if group:
                value = pltpu.roll(value, LANES - group * plan.series, 1)
            circle[pl.ds(source * plan.cols + first, count), :] = value
    circle[plan.total :, :] = jnp.zeros((circle.shape[0] - plan.total, LANES), jnp.float32)
    block = [circle[pl.ds(e * part, pad), :] for e in range(RADIX)]
    plus = [block[e] + block[e + 4] for e in range(4)]
    minus = [block[e] - block[e + 4] for e in range(4)]
    even, odd = plus[0] + plus[2], plus[1] + plus[3]
    root = math.sqrt(0.5)
    near, far = (minus[1] - minus[3]) * root, (minus[1] + minus[3]) * root
    inputs = (
        even + odd,
        even - odd,
        jnp.concatenate([minus[0] + near, -(minus[2] + far)], axis=0),
        jnp.concatenate([plus[0] - plus[2], plus[3] - plus[1]], axis=0),
        jnp.concatenate([minus[0] - near, minus[2] - far], axis=0),
    )
    cosine = cosine_ref[...]
    results = []
    for k in range(5):
        factor = cosine / jnp.maximum(CUT_COSINE * column_ref[:, k : k + 1], cosine)
        factor = factor * column_ref[:, 5 + k : 6 + k]
        if k >= 2:
            factor = jnp.concatenate([factor, factor], axis=0)
        table, at = (real_ref, k) if k < 2 else (mixed_ref, k - 2)
        spectrum = product(table, at, inputs[k], False) * factor
        results.append(product(table, at, spectrum, True))
    zero, four = results[0], results[1]
    one_r, one_i = results[2][:pad], results[2][pad:]
    two_r, two_i = results[3][:pad], results[3][pad:]
    three_r, three_i = results[4][:pad], results[4][pad:]
    mask = mask_ref[...] > 0
    same, swap = zero + four, zero - four
    s0, s2 = same + two_r, same - two_r
    s1, s3 = swap - two_i, swap + two_i
    d0 = one_r + three_r
    d2 = three_i - one_i
    p_r, p_i = (one_r - three_r) * root, (one_i + three_i) * root
    d1 = p_r - p_i
    d3 = -p_r - p_i
    outs = (s0 + d0, s1 + d1, s2 + d2, s3 + d3, s0 - d0, s1 - d1, s2 - d2, s3 - d3)
    for e in range(RADIX):
        value = (0.5 * jnp.where(mask, outs[e], block[e]))[:part]
        smooth[EDGE + e * part : EDGE + (e + 1) * part, :] = value
    tail = smooth.shape[0] - EDGE - plan.total
    smooth[EDGE - 1 : EDGE, :] = smooth[EDGE + plan.total - 1 : EDGE + plan.total, :]
    smooth[EDGE + plan.total :, :] = smooth[EDGE : EDGE + tail, :]
    lane = lax.broadcasted_iota(jnp.int32, (plan.in_rows, LANES), 1)
    for shift in range(devices):
        dest = lax.rem(me + shift, devices)
        start = EDGE - 1 + dest * plan.cols
        value = smooth[pl.ds(start, plan.in_rows), :]
        for group in range(1, plan.groups):
            other = smooth[pl.ds(start + group * plan.in_rows, plan.in_rows), :]
            other = pltpu.roll(other, group * plan.series, 1)
            value = jnp.where(lane >= group * plan.series, other, value)
        send_refs[shift][...] = value


def edge_kernel(tracers, first_ref, last_ref, sem):
    rows = tracers.shape[1]
    copies = []
    for side, (row, ref) in enumerate(((0, first_ref), (rows - 1, last_ref))):
        for k in range(ref.shape[0]):
            source = tracers.at[:, row, k * LANES : (k + 1) * LANES]
            copies.append(pltpu.make_async_copy(source, ref.at[k], sem.at[side, k]))
    for copy in copies:
        copy.start()
    for copy in copies:
        copy.wait()


def main_kernel(plan, group_cols, place_ref, tracers, west, east, south, north, rates_ref, *refs):
    devices, rows, cols = plan.devices, plan.rows, plan.cols
    recv_refs, (south_wind, north_wind, out) = refs[:devices], refs[devices : devices + 3]
    held, stage, wind, uspan, vspan, in_sem, out_sem = refs[devices + 3 :]
    tiles = tracers.shape[2] // LANES
    spread = tiles // MOMENTS
    groups = cols // group_cols
    deep = in_sem.shape[0] - 1
    stride = plan.in_rows + 1
    me = place_ref[0]
    open_s = place_ref[1].astype(jnp.float32)
    open_n = place_ref[2].astype(jnp.float32)
    body = slice(EDGE, EDGE + rows)

    def tile(k):
        return slice(k * LANES, (k + 1) * LANES)

    def load(g):
        at = lax.rem(g, deep)
        first = g * group_cols
        return [
            pltpu.make_async_copy(
                tracers.at[pl.ds(first, group_cols), :, tile(k)],
                held.at[k, pl.ds(first + 1, group_cols), body],
                in_sem.at[at, k],
            )
            for k in range(tiles)
        ]

    def load_side(source, slot, at):
        return [
            pltpu.make_async_copy(
                source.at[0, :, tile(k)], held.at[k, slot, body], in_sem.at[at, k]
            )
            for k in range(tiles)
        ]

    def store(g):
        slot = lax.rem(g, 2)
        return [
            pltpu.make_async_copy(
                stage.at[slot], out.at[pl.ds(g * group_cols, group_cols)], out_sem.at[slot]
            )
        ]

    def begin(copies):
        for copy in copies:
            copy.start()

    def finish(copies):
        for copy in copies:
            copy.wait()

    from_west = load_side(west, 0, deep)
    from_east = load_side(east, cols + 1, groups % deep)
    begin(from_west)
    for g in range(min(3, groups)):
        begin(load(g))

    for shift in range(devices):
        source = lax.rem(me - shift + devices, devices)
        wind[pl.ds(source * stride, plan.in_rows), :] = recv_refs[shift][...]
    wind[devices * stride : devices * stride + plan.in_rows, :] = south_wind[...]
    first = (devices + 1) * stride
    wind[first : first + plan.in_rows, :] = north_wind[...]

    lane = lax.broadcasted_iota(jnp.int32, (8, LANES), 1)
    sub = lax.broadcasted_iota(jnp.int32, (8, LANES), 0)

    def spread_levels(value, base):
        value = jnp.where((lane >= base) & (lane < base + LEV), value, 0.0)
        for step in (16, 32, 64):
            value = value + pltpu.roll(value, step, 1)
        return value

    def expand(at):
        group = sum((at >= k * plan.in_rows).astype(jnp.int32) for k in range(1, plan.groups))
        inside = at - group * plan.in_rows
        for block in range(rows // 8):
            for part, (span, lead) in enumerate(((uspan, 0), (vspan, EDGE))):
                source, base = plan.place(8 * block, part)
                value = wind[pl.ds(source * stride + inside, 8, stride=stride), :]
                value = spread_levels(value, group * plan.series + base)
                span[at, lead + 8 * block : lead + 8 * block + 8, :] = value
        _, base_s = plan.place(rows - 1, 1)
        _, base_n = plan.place(0, 1)
        value = wind[pl.ds(devices * stride + inside, 8, stride=stride), :]
        base = group * plan.series + jnp.where(sub == 0, base_s, base_n)
        value = spread_levels(value, base)
        vspan[at, EDGE - 1 : EDGE, :] = value[0:1]
        vspan[at, EDGE + rows : EDGE + rows + 1, :] = value[1:2]

    def fringe(c):
        slot = c + 1
        for k in range(tiles):
            held[k, slot, EDGE - 1 : EDGE, :] = south[k, pl.ds(c, 1), :]
            held[k, slot, EDGE + rows : EDGE + rows + 1, :] = north[k, pl.ds(c, 1), :]

    mask_s = jnp.where(lax.broadcasted_iota(jnp.int32, (rows, LANES), 0) == 0, open_s, 1.0)
    mask_n = jnp.where(
        lax.broadcasted_iota(jnp.int32, (rows, LANES), 0) == rows - 1, open_n, 1.0
    )

    def column(c, inner, slot):
        here, right, left = c + 1, c + 2, c
        u = uspan[c + 1]
        v = vspan[c + 1, body]
        se = u + uspan[c + 2]
        sw = u + uspan[c]
        sn = (v + vspan[c + 1, EDGE + 1 : EDGE + 1 + rows]) * mask_n
        ss = (v + vspan[c + 1, EDGE - 1 : EDGE - 1 + rows]) * mask_s
        ce, cw = jnp.minimum(se, 0.0), jnp.maximum(sw, 0.0)
        cn, cs = jnp.minimum(sn, 0.0), jnp.maximum(ss, 0.0)
        cc = ((1.0 - (se - sw)) - (sn - ss)) + ((ce - cw) + (cn - cs))
        for part in range(spread):
            moments = []
            for degree in range(MOMENTS):
                k = degree * spread + part
                value = cc * held[k, here, body]
                value = value - ce * held[k, right, body]
                value = value + cw * held[k, left, body]
                value = value - cn * held[k, here, EDGE + 1 : EDGE + 1 + rows]
                value = value + cs * held[k, here, EDGE - 1 : EDGE - 1 + rows]
                moments.append(value)
            coag = rates_ref[part : part + 1, :]
            growths = [
                rates_ref[(1 + k) * spread + part : (1 + k) * spread + part + 1, :]
                for k in range(MOMENTS - 1)
            ]
            result = moment_update(moments, coag, growths)
            for degree in range(MOMENTS):
                stage[slot, inner, :, tile(degree * spread + part)] = result[degree]

    pl.loop(0, STEP + 2)(expand)
    pl.loop(0, STEP)(fringe)
    finish(from_west)
    finish(load(0))

    @pl.loop(0, groups)
    def _(g):
        slot = lax.rem(g, 2)

        @pl.when(g + 3 < groups)
        def _():
            begin(load(g + 3))

        @pl.when(g + 3 == groups)
        def _():
            begin(from_east)

        @pl.when(g + 1 < groups)
        def _():
            finish(load(g + 1))

        @pl.when(g + 1 == groups)
        def _():
            finish(from_east)

        @pl.when(g >= 2)
        def _():
            finish(store(g - 2))

        @pl.loop(0, group_cols // STEP)
        def _(i):
            first = g * group_cols + i * STEP
            for step in range(STEP):
                column(first + step, i * STEP + step, slot)
            for step in range(STEP):
                expand(jnp.minimum(first + STEP + 2 + step, cols + 1))
                fringe(jnp.minimum(first + STEP + step, cols - 1))

        begin(store(g))

    for g in range(max(0, groups - 2), groups):
        finish(store(g))


VMEM = pl.BlockSpec(memory_space=pltpu.VMEM)
SMEM = pl.BlockSpec(memory_space=pltpu.SMEM)
ANY = pl.BlockSpec(memory_space=pl.ANY)
PARAMS = pltpu.CompilerParams(vmem_limit_bytes=60 * 1024 * 1024)


def ring(devices, shift):
    return [(i, (i + shift) % devices) for i in range(devices)]


def exchange(pieces, devices):
    return [
        piece if s == 0 else lax.ppermute(piece, "lon", ring(devices, s))
        for s, piece in enumerate(pieces)
    ]


def row_angles(places):
    return (-90.0 + 180.0 * (places.astype(jnp.float32) + 0.5) / GLOBE_ROWS) * (math.pi / 180.0)


def local(tracers, winds, row_mask, coag_rate, growth_rate):
    rows, cols, width = tracers.shape
    channels = winds.shape[2]
    bands, sectors = lax.axis_size("lat"), lax.axis_size("lon")
    band, me = lax.axis_index("lat"), lax.axis_index("lon")
    plan = Plan(rows, cols, sectors, channels)
    tiles = width // LANES
    spread = tiles // MOMENTS
    f32 = jnp.float32
    place = jnp.stack([me, band > 0, band < bands - 1]).astype(jnp.int32)
    turned = tracers.transpose(1, 0, 2)

    up = [(i, i + 1) for i in range(bands - 1)]
    down = [(i + 1, i) for i in range(bands - 1)]
    strip = jax.ShapeDtypeStruct((tiles, cols, LANES), f32)
    first_row, last_row = pl.pallas_call(
        edge_kernel,
        out_shape=[strip] * 2,
        in_specs=[ANY],
        out_specs=[VMEM] * 2,
        scratch_shapes=[pltpu.SemaphoreType.DMA((2, tiles))],
        compiler_params=PARAMS,
        name="edge_rows",
    )(turned)
    winds, first_row, last_row = lax.optimization_barrier((winds, first_row, last_row))
    south = lax.ppermute(last_row, "lat", up)
    north = lax.ppermute(first_row, "lat", down)

    sent = jax.ShapeDtypeStruct((plan.out_rows, LANES), f32)
    pieces = pl.pallas_call(
        functools.partial(pack_kernel, plan),
        out_shape=[sent] * sectors,
        in_specs=[SMEM, VMEM],
        out_specs=[VMEM] * sectors,
        scratch_shapes=[pltpu.VMEM((cols, LANES), f32)],
        compiler_params=PARAMS,
        name="pack",
    )(place, winds.transpose(0, 2, 1))
    pieces = exchange(pieces, sectors)


    west = lax.ppermute(turned[cols - 1 :], "lon", ring(sectors, 1))
    east = lax.ppermute(turned[:1], "lon", ring(sectors, sectors - 1))

    real, mixed, columns, pad = class_tables(plan.total)
    lane_row = plan.row_of(me, jnp.arange(LANES, dtype=jnp.int32) % plan.series)
    cosines = jnp.cos(row_angles(band * rows + lane_row))[None, :]
    chosen = (lane_row[:, None] == jnp.arange(rows, dtype=jnp.int32)[None, :]).astype(jnp.int32)
    mask = jnp.sum(chosen * row_mask[None, :], axis=1)[None, :]
    back = jax.ShapeDtypeStruct((plan.in_rows, LANES), f32)
    part = plan.total // RADIX
    reach = plan.total + plan.groups * plan.in_rows
    filtered = pl.pallas_call(
        functools.partial(filter_kernel, plan, pad),
        out_shape=[back] * sectors,
        in_specs=[SMEM] + [VMEM] * (5 + sectors),
        out_specs=[VMEM] * sectors,
        scratch_shapes=[
            pltpu.VMEM((round_up(plan.total - part + pad, 8), LANES), f32),
            pltpu.VMEM((EDGE + round_up(reach - plan.cols, 8), LANES), f32),
        ],
        compiler_params=PARAMS,
        name="filter",
    )(place, real, mixed, columns, cosines, mask, *pieces)
    filtered = exchange(filtered, sectors)

    def block_of(row):
        owner, _ = plan.place(row, 1)
        shift = lax.rem(me - owner + sectors, sectors)
        value = filtered[0]
        for s in range(1, sectors):
            value = jnp.where(shift == s, filtered[s], value)
        return value

    south_wind = lax.ppermute(block_of(rows - 1), "lat", up)
    north_wind = lax.ppermute(block_of(0), "lat", down)

    coag = jnp.repeat(coag_rate, LEV).reshape(spread, LANES)
    growth = jnp.repeat(growth_rate, LEV).reshape(spread, LANES)
    order = jnp.arange(MOMENTS, dtype=jnp.int32)[:, None, None]
    rates = jnp.where(order == 0, coag[None], order.astype(f32) * growth[None])
    rates = rates.reshape(MOMENTS * spread, LANES)

    group_cols = max(k for k in range(1, GROUP + 1) if cols % k == 0 and k % STEP == 0)
    deep = 4
    stride = plan.in_rows + 1
    result = pl.pallas_call(
        functools.partial(main_kernel, plan, group_cols),
        out_shape=jax.ShapeDtypeStruct(turned.shape, f32),
        in_specs=[SMEM] + [ANY] * 3 + [VMEM] * (5 + sectors),
        out_specs=ANY,
        scratch_shapes=[
            pltpu.VMEM((tiles, cols + 2, rows + 2 * EDGE, LANES), f32),
            pltpu.VMEM((2, group_cols, rows, width), f32),
            pltpu.VMEM((round_up((sectors + 8) * stride, 8), LANES), f32),
            pltpu.VMEM((cols + 2, rows, LANES), f32),
            pltpu.VMEM((cols + 2, rows + 2 * EDGE, LANES), f32),
            pltpu.SemaphoreType.DMA((deep + 1, tiles)),
            pltpu.SemaphoreType.DMA((2,)),
        ],
        cost_estimate=pl.CostEstimate(
            flops=turned.size * 100, bytes_accessed=turned.size * 8, transcendentals=0
        ),
        compiler_params=pltpu.CompilerParams(vmem_limit_bytes=60 * 1024 * 1024),
        name="update",
    )(place, turned, west, east, south, north, rates, *filtered, south_wind, north_wind)
    return result.transpose(1, 0, 2)


def solution(mesh):
    in_specs = (P("lat", "lon", None), P("lat", "lon", None), P("lat"), P(), P())
    out_specs = P("lat", "lon", None)

    return jax.shard_map(local, mesh=mesh, in_specs=in_specs, out_specs=out_specs, check_vma=False)
```
